32 devices in a mesh: shot: 2 (over x), mp: 16 (over z, y, core).
Axes of the slice: x: 2, y: 2, z: 4, core: 2. Of those that a mesh axis runs over, the one named last changes fastest.
Arguments:
- gradient_parts: float32 [8, 1024, 1024], P('shot', 'mp')
- history_s: bfloat16 [10, 1024, 1024], P(None, 'mp'), may hold values from -6 to 6
- history_y: bfloat16 [10, 1024, 1024], P(None, 'mp'), as said below
Outputs:
- direction: float32 [1024, 1024], P('mp', 'shot')
The draws below stay inside these ranges and needn't reach their ends.
Inputs may be any that keep to these rules, and one draw needn't show every extreme that they name: In every cell, history_y[i] equals history_s[i] times a factor between 0.5 and 4.
All inputs are finite; a program needn't handle non-finite values.
Results may differ from the reference program's by a relative error of at most 0.0003.
Values sent between devices are 32-bit elements; how exact they have to be, the bound alone decides.
A program may use at most 64 MiB of HBM per device.

```python
import jax
import jax.numpy as jnp
from jax import lax

M = 10
SHOT_DEV = 4
WIDTH = 1024
ROWS = 1024
N_SHOT = 2


def basis(key):
    keys = jax.random.split(jax.random.fold_in(key, 11), 2)
    ramp = jnp.exp(jnp.log(3.0) * jnp.arange(ROWS, dtype=jnp.float32) / (ROWS - 1))[None, :, None]
    steps = jnp.clip(jax.random.normal(keys[0], (M, ROWS, WIDTH), jnp.float32), -2.0, 2.0)
    steps = steps * ramp
    factor = jnp.exp(jax.random.uniform(keys[1], (M, ROWS, WIDTH), jnp.float32, -0.69, 1.38))
    return (steps, factor * steps)


def draw_history_s(key, part):
    return basis(key)[0].astype(jnp.bfloat16)


def draw_history_y(key, part):
    return basis(key)[1].astype(jnp.bfloat16)


def draw_gradient_parts(key, part):
    steps, changes = basis(key)
    keys = jax.random.split(jax.random.fold_in(key, 23), 3)
    mix_s = jax.random.normal(keys[0], (M,), jnp.float32) / (2.0 * M) ** 0.5
    mix_y = jax.random.normal(keys[1], (M,), jnp.float32) / (2.0 * M) ** 0.5
    common = jnp.einsum('m,mrc->rc', mix_s, steps, precision=lax.Precision.HIGHEST)
    common = common + jnp.einsum('m,mrc->rc', mix_y, changes, precision=lax.Precision.HIGHEST)
    total = SHOT_DEV * N_SHOT
    ramp = 1.0 + 2.0 * jnp.arange(total, dtype=jnp.float32) / (total - 1)
    noise = jax.random.normal(keys[2], (total, ROWS, WIDTH), jnp.float32)
    return ramp[:, None, None] * (common[None] / total + 0.5 / total ** 0.5 * noise)


def setup_inputs(seed: int = 0) -> dict:
    splits = jax.random.split(jax.random.key(seed), 4)
    return {
        "gradient_parts": draw_gradient_parts(jax.random.fold_in(splits[3], 71), 0),
        "history_s": draw_history_s(jax.random.fold_in(splits[3], 71), 0),
        "history_y": draw_history_y(jax.random.fold_in(splits[3], 71), 0),
    }


def inner(left, right):
    return jnp.sum(left.astype(jnp.float32) * right.astype(jnp.float32))


def reference(gradient_parts, history_s, history_y):
    gradient = jnp.sum(gradient_parts, axis=0)
    rho = [1.0 / inner(history_s[i], history_y[i]) for i in range(M)]
    gamma = inner(history_s[M - 1], history_y[M - 1]) / inner(history_y[M - 1], history_y[M - 1])
    q_vec = gradient
    alphas = [None] * M
    for i in reversed(range(M)):
        alphas[i] = rho[i] * inner(history_s[i], q_vec)
        q_vec = q_vec - alphas[i] * history_y[i].astype(jnp.float32)
    r_vec = gamma * q_vec
    for i in range(M):
        beta = rho[i] * inner(history_y[i], r_vec)
        r_vec = r_vec + (alphas[i] - beta) * history_s[i].astype(jnp.float32)
    return -r_vec
```

```python
import functools

import jax
import jax.numpy as jnp
from jax import lax
from jax.experimental import pallas as pl
from jax.experimental.pallas import tpu as pltpu
from jax.sharding import PartitionSpec as P

M = 10
G = 16
MESH = pl.DeviceIdType.MESH


def place(a, b):
    return a % 8, G * (b % 8) + (a // 8) * 2 + b // 8


def pack(acc, n_shot):
    lanes = acc.shape[1]
    row = lax.broadcasted_iota(jnp.int32, acc.shape, 0) % G
    col = lax.broadcasted_iota(jnp.int32, acc.shape, 1) % G
    kept = jnp.where(row == col, acc, 0.0)
    sums = jnp.sum(kept.reshape(2 * M, G, lanes), axis=1)
    sums = jnp.concatenate([sums, jnp.zeros((24 - 2 * M, lanes), jnp.float32)], axis=0)
    for shift in (8, 4, 2, 1):
        sums = sums + pltpu.roll(sums, lanes - shift, 1)
    wide = sums + pltpu.roll(sums, lanes - G, 1) + pltpu.roll(sums, lanes - 2 * G, 1)
    group = lax.broadcasted_iota(jnp.int32, sums.shape, 1) // G
    sums = jnp.where(group == M, wide, sums * (1.0 / n_shot))
    lane = lax.broadcasted_iota(jnp.int32, (8, 128), 1) % G
    packed = jnp.zeros((8, 128), jnp.float32)
    for p in range(3):
        for q in range(2):
            piece = sums[8 * p : 8 * p + 8, 128 * q : 128 * q + 128]
            index = 2 * p + q
            if index:
                piece = pltpu.roll(piece, index, 1)
            packed = jnp.where(lane == index, piece, packed)
    return packed


def two_loop(get, inv):
    alphas = [None] * M
    left = [get(i, M) for i in range(M)]
    for j in reversed(range(M)):
        alphas[j] = left[j] * inv(j, j)
        for i in range(j):
            left[i] = left[i] - alphas[j] * get(i, j)
    gamma = get(M - 1, M - 1) * inv(2 * M - 1, M - 1)
    moved = []
    for i in range(M):
        dot = get(M + i, M)
        for j in range(M):
            dot = dot - alphas[j] * get(M + i, j)
        moved.append(gamma * dot)
    deltas = [None] * M
    for i in range(M):
        deltas[i] = alphas[i] - moved[i] * inv(i, i)
        for k in range(i + 1, M):
            moved[k] = moved[k] + deltas[i] * get(i, k)
    return deltas, [-gamma * a for a in alphas], gamma


def kernel(
    n_shot, n_mp, parts_hbm, s_hbm, y_hbm, out_ref,
    parts, s_all, y_all, partial, others, acc, mine, blocks, half, halves, scalars, tot,
    in_sem, g_send, g_recv, a_send, a_recv, b_send, b_recv, s_sem,
):
    shot, mp = lax.axis_index("shot"), lax.axis_index("mp")
    rows, width = parts.shape[1], parts.shape[2]
    cols = width // n_shot
    groups = rows // G

    def load(hbm, vmem, which, r):
        span = pl.ds(r * G, G)
        return pltpu.make_async_copy(hbm.at[:, span, :], vmem.at[:, span, :], in_sem.at[which, r])

    loads = []
    for r in range(groups):
        loads.append((load(parts_hbm, parts, 0, r), load(s_hbm, s_all, 1, r), load(y_hbm, y_all, 2, r)))
        for copy in loads[-1]:
            copy.start()

    barrier = pltpu.get_barrier_semaphore()
    for k in range(1, n_mp):
        pl.semaphore_signal(barrier, inc=1, device_id={"mp": lax.rem(mp + k, n_mp)}, device_id_type=MESH)
    for k in range(1, n_shot):
        pl.semaphore_signal(barrier, inc=1, device_id={"shot": lax.rem(shot + k, n_shot)}, device_id_type=MESH)

    for r in range(groups):
        for copy in loads[r]:
            copy.wait()
        span = slice(r * G, r * G + G)
        grad = parts[0, span, :]
        for i in range(1, parts.shape[0]):
            grad = grad + parts[i, span, :]
        for p in range(n_shot):
            partial[p, span, :] = grad[:, p * cols : p * cols + cols]
        high = grad.astype(jnp.bfloat16)
        rest = grad - high.astype(jnp.float32)
        mid = rest.astype(jnp.bfloat16)
        low = (rest - mid.astype(jnp.float32)).astype(jnp.bfloat16)
        s = s_all[:, span, :].reshape(M * G, width)
        y = y_all[:, span, :].reshape(M * G, width)
        left = jnp.concatenate([s, y], axis=0)
        right = jnp.concatenate([y, high, mid, low, jnp.zeros((3 * G, width), jnp.bfloat16)], axis=0)
        prod = lax.dot_general(left, right, (((1,), (1,)), ((), ())), preferred_element_type=jnp.float32)
        if r == 0:
            acc[...] = prod
        else:
            acc[...] += prod

    pl.semaphore_wait(barrier, n_mp + n_shot - 2)
    g_copies = []
    for k in range(1, n_shot):
        to = lax.rem(shot + k, n_shot)
        copy = pltpu.make_async_remote_copy(
            src_ref=partial.at[to], dst_ref=others.at[shot], send_sem=g_send.at[k], recv_sem=g_recv.at[shot],
            device_id={"shot": to}, device_id_type=MESH,
        )
        copy.start()
        g_copies.append(copy)

    packed = pack(acc[...], n_shot)
    mine[...] = packed

    def spread(src, dst, axis, me, n, send, recv):
        copies = []
        for k in range(1, n):
            copy = pltpu.make_async_remote_copy(
                src_ref=src, dst_ref=dst.at[me], send_sem=send.at[k], recv_sem=recv.at[me],
                device_id={axis: lax.rem(me + k, n)}, device_id_type=MESH,
            )
            copy.start()
            copies.append(copy)
        return copies

    def arrive(src, dst, axis, me, n, send, recv):
        for k in range(1, n):
            frm = lax.rem(me + k, n)
            pltpu.make_async_remote_copy(
                src_ref=src, dst_ref=dst.at[frm], send_sem=send.at[k], recv_sem=recv.at[frm],
                device_id={axis: frm}, device_id_type=MESH,
            ).wait_recv()

    a_copies = spread(mine, blocks, "mp", mp, n_mp, a_send, a_recv)
    blocks[mp] = packed
    arrive(mine, blocks, "mp", mp, n_mp, a_send, a_recv)
    total = blocks[0]
    for p in range(1, n_mp):
        total = total + blocks[p]
    half[...] = total
    b_copies = spread(half, halves, "shot", shot, n_shot, b_send, b_recv)
    halves[shot] = total
    arrive(half, halves, "shot", shot, n_shot, b_send, b_recv)
    total = halves[0]
    for p in range(1, n_shot):
        total = total + halves[p]
    tot[0] = total
    tot[1] = 1.0 / total
    copy = pltpu.make_async_copy(tot, scalars, s_sem)
    copy.start()
    copy.wait()

    def get(a, b):
        i, j = place(a, b)
        return scalars[0, i, j]

    def inv(a, b):
        i, j = place(a, b)
        return scalars[1, i, j]

    c_s, c_y, c_g = two_loop(get, inv)
    for k in range(1, n_shot):
        frm = lax.rem(shot + k, n_shot)
        pltpu.make_async_remote_copy(
            src_ref=partial.at[frm], dst_ref=others.at[frm], send_sem=g_send.at[k], recv_sem=g_recv.at[frm],
            device_id={"shot": frm}, device_id_type=MESH,
        ).wait_recv()
    own = pl.ds(pl.multiple_of(shot * cols, cols), cols)
    for r in range(groups):
        span = slice(r * G, r * G + G)
        grad = partial[shot, span, :]
        for k in range(1, n_shot):
            grad = grad + others[lax.rem(shot + k, n_shot), span, :]
        result = -c_g * grad
        for i in range(M):
            result = result - c_y[i] * y_all[i, span, own].astype(jnp.float32)
            result = result - c_s[i] * s_all[i, span, own].astype(jnp.float32)
        out_ref[span, :] = result
    for copy in g_copies + a_copies + b_copies:
        copy.wait_send()


def solution(mesh):
    n_shot, n_mp = mesh.shape["shot"], mesh.shape["mp"]

    def step(parts, s, y):
        shots, rows, width = parts.shape
        cols = width // n_shot
        dma = pltpu.SemaphoreType.DMA
        return pl.pallas_call(
            functools.partial(kernel, n_shot, n_mp),
            out_shape=jax.ShapeDtypeStruct((rows, cols), jnp.float32),
            in_specs=[pl.BlockSpec(memory_space=pl.ANY)] * 3,
            out_specs=pl.BlockSpec(memory_space=pltpu.VMEM),
            scratch_shapes=[
                pltpu.VMEM((shots, rows, width), jnp.float32),
                pltpu.VMEM((M, rows, width), jnp.bfloat16),
                pltpu.VMEM((M, rows, width), jnp.bfloat16),
                pltpu.VMEM((n_shot, rows, cols), jnp.float32),
                pltpu.VMEM((n_shot, rows, cols), jnp.float32),
                pltpu.VMEM((2 * M * G, 256), jnp.float32),
                pltpu.VMEM((8, 128), jnp.float32),
                pltpu.VMEM((n_mp, 8, 128), jnp.float32),
                pltpu.VMEM((8, 128), jnp.float32),
                pltpu.VMEM((n_shot, 8, 128), jnp.float32),
                pltpu.SMEM((2, 8, 128), jnp.float32),
                pltpu.VMEM((2, 8, 128), jnp.float32),
                dma((3, rows // G)),
                dma((n_shot,)),
                dma((n_shot,)),
                dma((n_mp,)),
                dma((n_mp,)),
                dma((n_shot,)),
                dma((n_shot,)),
                dma,
            ],
            compiler_params=pltpu.CompilerParams(collective_id=0, has_side_effects=True),
        )(parts, s, y)

    placed = (P("shot", "mp", None), P(None, "mp", None), P(None, "mp", None))
    return jax.shard_map(step, mesh=mesh, in_specs=placed, out_specs=P("mp", "shot"), check_vma=False)
```

```python
import functools

import jax
import jax.numpy as jnp
from jax import lax
from jax.experimental import pallas as pl
from jax.experimental.pallas import tpu as pltpu
from jax.sharding import PartitionSpec as P

M = 10
G = 16
MESH = pl.DeviceIdType.MESH


def place(a, b):
    return a % 8, G * (b % 8) + (a // 8) * 2 + b // 8


def pack(acc, n_shot):
    lanes = acc.shape[1]
    row = lax.broadcasted_iota(jnp.int32, acc.shape, 0) % G
    col = lax.broadcasted_iota(jnp.int32, acc.shape, 1) % G
    kept = jnp.where(row == col, acc, 0.0)
    sums = jnp.sum(kept.reshape(2 * M, G, lanes), axis=1)
    sums = jnp.concatenate([sums, jnp.zeros((24 - 2 * M, lanes), jnp.float32)], axis=0)
    for shift in (8, 4, 2, 1):
        sums = sums + pltpu.roll(sums, lanes - shift, 1)
    wide = sums + pltpu.roll(sums, lanes - G, 1) + pltpu.roll(sums, lanes - 2 * G, 1)
    group = lax.broadcasted_iota(jnp.int32, sums.shape, 1) // G
    sums = jnp.where(group == M, wide, sums * (1.0 / n_shot))
    lane = lax.broadcasted_iota(jnp.int32, (8, 128), 1) % G
    packed = jnp.zeros((8, 128), jnp.float32)
    for p in range(3):
        for q in range(2):
            piece = sums[8 * p : 8 * p + 8, 128 * q : 128 * q + 128]
            index = 2 * p + q
            if index:
                piece = pltpu.roll(piece, index, 1)
            packed = jnp.where(lane == index, piece, packed)
    return packed


def two_loop(get, inv):
    alphas = [None] * M
    left = [get(i, M) for i in range(M)]
    for j in reversed(range(M)):
        alphas[j] = left[j] * inv(j, j)
        for i in range(j):
            left[i] = left[i] - alphas[j] * get(i, j)
    gamma = get(M - 1, M - 1) * inv(2 * M - 1, M - 1)
    moved = []
    for i in range(M):
        dot = get(M + i, M)
        for j in range(M):
            dot = dot - alphas[j] * get(M + i, j)
        moved.append(gamma * dot)
    deltas = [None] * M
    for i in range(M):
        deltas[i] = alphas[i] - moved[i] * inv(i, i)
        for k in range(i + 1, M):
            moved[k] = moved[k] + deltas[i] * get(i, k)
    return deltas, [-gamma * a for a in alphas], gamma


def kernel(
    n_shot, n_mp, parts_hbm, s_hbm, y_hbm, out_ref,
    parts, s_all, y_all, partial, others, acc, mine, blocks, scalars, tot,
    in_sem, g_send, g_recv, a_send, a_recv, s_sem,
):
    shot, mp = lax.axis_index("shot"), lax.axis_index("mp")
    rows, width = parts.shape[1], parts.shape[2]
    cols = width // n_shot
    groups = rows // G

    def load(hbm, vmem, which, r):
        span = pl.ds(r * G, G)
        return pltpu.make_async_copy(hbm.at[:, span, :], vmem.at[:, span, :], in_sem.at[which, r])

    sources = ((parts_hbm, parts), (s_hbm, s_all), (y_hbm, y_all))
    loads = [[load(*sources[w], w, r) for w in range(3)] for r in range(groups)]
    for r in range(groups):
        loads[r][0].start()
    for r in range(groups):
        loads[r][1].start()
        loads[r][2].start()

    barrier = pltpu.get_barrier_semaphore()
    for d in range(n_shot):
        for k in range(n_mp):
            if d or k:
                to = {"shot": lax.rem(shot + d, n_shot), "mp": lax.rem(mp + k, n_mp)}
                pl.semaphore_signal(barrier, inc=1, device_id=to, device_id_type=MESH)

    for r in range(groups):
        loads[r][0].wait()
        span = slice(r * G, r * G + G)
        for p in range(n_shot):
            part = slice(p * cols, p * cols + cols)
            grad = parts[0, span, part]
            for i in range(1, parts.shape[0]):
                grad = grad + parts[i, span, part]
            partial[p, span, :] = grad

    for r in range(0, groups - 2):
        loads[r][1].wait()
        loads[r][2].wait()
        span = slice(r * G, r * G + G)
        grad = jnp.concatenate([partial[p, span, :] for p in range(n_shot)], axis=1)
        high = grad.astype(jnp.bfloat16)
        rest = grad - high.astype(jnp.float32)
        mid = rest.astype(jnp.bfloat16)
        low = (rest - mid.astype(jnp.float32)).astype(jnp.bfloat16)
        s = s_all[:, span, :].reshape(M * G, width)
        y = y_all[:, span, :].reshape(M * G, width)
        left = jnp.concatenate([s, y], axis=0)
        right = jnp.concatenate([y, high, mid, low, jnp.zeros((3 * G, width), jnp.bfloat16)], axis=0)
        prod = lax.dot_general(left, right, (((1,), (1,)), ((), ())), preferred_element_type=jnp.float32)
        if r == 0:
            acc[...] = prod
        else:
            acc[...] += prod

    pl.semaphore_wait(barrier, n_mp * n_shot - 1)
    g_copies = []
    for k in range(1, n_shot):
        to = lax.rem(shot + k, n_shot)
        copy = pltpu.make_async_remote_copy(
            src_ref=partial.at[to], dst_ref=others.at[shot], send_sem=g_send.at[k], recv_sem=g_recv.at[shot],
            device_id={"shot": to}, device_id_type=MESH,
        )
        copy.start()
        g_copies.append(copy)

    for r in range(groups - 2, groups):
        loads[r][1].wait()
        loads[r][2].wait()
        span = slice(r * G, r * G + G)
        grad = jnp.concatenate([partial[p, span, :] for p in range(n_shot)], axis=1)
        high = grad.astype(jnp.bfloat16)
        rest = grad - high.astype(jnp.float32)
        mid = rest.astype(jnp.bfloat16)
        low = (rest - mid.astype(jnp.float32)).astype(jnp.bfloat16)
        s = s_all[:, span, :].reshape(M * G, width)
        y = y_all[:, span, :].reshape(M * G, width)
        left = jnp.concatenate([s, y], axis=0)
        right = jnp.concatenate([y, high, mid, low, jnp.zeros((3 * G, width), jnp.bfloat16)], axis=0)
        prod = lax.dot_general(left, right, (((1,), (1,)), ((), ())), preferred_element_type=jnp.float32)
        if r == 0:
            acc[...] = prod
        else:
            acc[...] += prod

    packed = pack(acc[...], n_shot)
    mine[...] = packed

    here = shot * n_mp + mp
    a_copies = []
    for d in range(n_shot):
        for k in range(n_mp):
            if d or k:
                copy = pltpu.make_async_remote_copy(
                    src_ref=mine, dst_ref=blocks.at[here], send_sem=a_send.at[d, k], recv_sem=a_recv.at[here],
                    device_id={"shot": lax.rem(shot + d, n_shot), "mp": lax.rem(mp + k, n_mp)}, device_id_type=MESH,
                )
                copy.start()
                a_copies.append(copy)
    blocks[here] = packed
    for d in range(n_shot):
        for k in range(n_mp):
            if d or k:
                row, col = lax.rem(shot + d, n_shot), lax.rem(mp + k, n_mp)
                frm = row * n_mp + col
                pltpu.make_async_remote_copy(
                    src_ref=mine, dst_ref=blocks.at[frm], send_sem=a_send.at[d, k], recv_sem=a_recv.at[frm],
                    device_id={"shot": row, "mp": col}, device_id_type=MESH,
                ).wait_recv()
    total = blocks[0]
    for p in range(1, n_shot * n_mp):
        total = total + blocks[p]
    tot[0] = total
    tot[1] = 1.0 / total
    copy = pltpu.make_async_copy(tot, scalars, s_sem)
    copy.start()
    copy.wait()

    def get(a, b):
        i, j = place(a, b)
        return scalars[0, i, j]

    def inv(a, b):
        i, j = place(a, b)
        return scalars[1, i, j]

    c_s, c_y, c_g = two_loop(get, inv)
    for k in range(1, n_shot):
        frm = lax.rem(shot + k, n_shot)
        pltpu.make_async_remote_copy(
            src_ref=partial.at[frm], dst_ref=others.at[frm], send_sem=g_send.at[k], recv_sem=g_recv.at[frm],
            device_id={"shot": frm}, device_id_type=MESH,
        ).wait_recv()
    own = pl.ds(pl.multiple_of(shot * cols, cols), cols)
    for r in range(groups):
        span = slice(r * G, r * G + G)
        grad = partial[shot, span, :]
        for k in range(1, n_shot):
            grad = grad + others[lax.rem(shot + k, n_shot), span, :]
        result = -c_g * grad
        for i in range(M):
            result = result - c_y[i] * y_all[i, span, own].astype(jnp.float32)
            result = result - c_s[i] * s_all[i, span, own].astype(jnp.float32)
        out_ref[span, :] = result
    for copy in g_copies + a_copies:
        copy.wait_send()


def solution(mesh):
    n_shot, n_mp = mesh.shape["shot"], mesh.shape["mp"]

    def step(parts, s, y):
        shots, rows, width = parts.shape
        cols = width // n_shot
        dma = pltpu.SemaphoreType.DMA
        return pl.pallas_call(
            functools.partial(kernel, n_shot, n_mp),
            out_shape=jax.ShapeDtypeStruct((rows, cols), jnp.float32),
            in_specs=[pl.BlockSpec(memory_space=pl.ANY)] * 3,
            out_specs=pl.BlockSpec(memory_space=pltpu.VMEM),
            scratch_shapes=[
                pltpu.VMEM((shots, rows, width), jnp.float32),
                pltpu.VMEM((M, rows, width), jnp.bfloat16),
                pltpu.VMEM((M, rows, width), jnp.bfloat16),
                pltpu.VMEM((n_shot, rows, cols), jnp.float32),
                pltpu.VMEM((n_shot, rows, cols), jnp.float32),
                pltpu.VMEM((2 * M * G, 256), jnp.float32),
                pltpu.VMEM((8, 128), jnp.float32),
                pltpu.VMEM((n_shot * n_mp, 8, 128), jnp.float32),
                pltpu.SMEM((2, 8, 128), jnp.float32),
                pltpu.VMEM((2, 8, 128), jnp.float32),
                dma((3, rows // G)),
                dma((n_shot,)),
                dma((n_shot,)),
                dma((n_shot, n_mp)),
                dma((n_shot * n_mp,)),
                dma,
            ],
            compiler_params=pltpu.CompilerParams(collective_id=0, has_side_effects=True, vmem_limit_bytes=56_000_000),
        )(parts, s, y)

    placed = (P("shot", "mp", None), P(None, "mp", None), P(None, "mp", None))
    return jax.shard_map(step, mesh=mesh, in_specs=placed, out_specs=P("mp", "shot"), check_vma=False)
```
